32 devices in a mesh: blk: 32 (over z, y, x, core).
Axes of the slice: x: 2, y: 2, z: 4, core: 2. Of those that a mesh axis runs over, the one named last changes fastest.
Arguments:
- frames: float32 [128, 128, 1280], P('blk'), may hold values from -6 to 6
- widths: float32 [128], replicated, may hold values from 2 to 12
- kernel: float32 [3, 3], replicated, may hold values from -3 to 3
Outputs:
- filtered: float32 [128, 128, 1280], P(None, 'blk')
The draws below stay inside these ranges and needn't reach their ends.
All inputs are finite; a program needn't handle non-finite values.
Results may differ from the reference program's by a relative error of at most 0.00007.
Values sent between devices are 32-bit elements; how exact they have to be, the bound alone decides.
No kernel may reach another device: no remote copies, remote signals or barrier semaphores. Data moves between devices by JAX's collectives and lax.ppermute only.
A program may use at most 64 MiB of HBM per device.

```python
import math
import jax
import jax.numpy as jnp
from jax import lax

FRAMES = 128
BAND = 24
W = 1280
H = 128


def block_scale(key, shape, pieces, least, top_value):
    factor_of, own = 1.0, jax.random.fold_in(key, 6)
    for axis_at, shards_of in pieces:
        heights = jnp.exp(jax.random.uniform(jax.random.fold_in(own, axis_at), (shards_of,), jnp.float32, least / len(pieces), top_value / len(pieces)))
        factor_of = factor_of * jnp.repeat(heights, shape[axis_at] // shards_of).reshape([-1 if axis == axis_at else 1 for axis in range(len(shape))])
    return factor_of


def normal_values(key, extent, scale, most, cuts=(), kind=jnp.bfloat16):
    values = scale * jax.random.normal(key, extent, jnp.float32)
    if cuts:
        values = values * block_scale(key, extent, cuts, -0.22, 0.18)
    return jnp.clip(values, -most, most).astype(kind)


def setup_inputs(seed: int = 0) -> dict:
    key_of = jax.random.split(jax.random.key(seed), 4)
    frames = normal_values(key_of[0], (FRAMES, H, W), 1.0, 6.0, ((0, 32),), jnp.float32)
    widths = jnp.clip(jnp.exp(jax.random.uniform(key_of[1], (FRAMES,), jnp.float32, math.log(2.0), math.log(12.0))), 2.0, 12.0)
    kernel = normal_values(key_of[2], (3, 3), 0.5, 3.0, (), jnp.float32)
    return dict(frames=frames, widths=widths, kernel=kernel)


def temporal_matrix(widths, length):
    steps = jnp.arange(length, dtype=jnp.int32)
    offset = (steps[:, None] - steps[None, :]).astype(jnp.float32)
    inside = jnp.abs(offset) <= BAND
    spread = widths.astype(jnp.float32)[:, None]
    weights = jnp.where(inside, jnp.exp(-offset * offset / (2.0 * spread * spread)), 0.0)
    return weights / jnp.sum(weights, axis=1, keepdims=True)


def stencil(padded, kernel):
    rows_out = padded.shape[1] - 2
    columns = padded.shape[2]
    widened = jnp.pad(padded, ((0, 0), (0, 0), (1, 1)))
    summed = jnp.zeros((padded.shape[0], rows_out, columns), jnp.float32)
    for row_off in range(3):
        for col_off in range(3):
            summed = summed + kernel[row_off, col_off] * widened[:, row_off:row_off + rows_out, col_off:col_off + columns]
    return summed


def reference(frames, widths, kernel):
    weights = temporal_matrix(widths, frames.shape[0])
    smoothed = jnp.einsum("ts,srw->trw", weights, frames, precision=lax.Precision.HIGHEST)
    padded = jnp.pad(smoothed, ((0, 0), (1, 1), (0, 0)))
    return stencil(padded, kernel)
```

```python
import functools

import jax
import jax.numpy as jnp
from jax import lax
from jax.experimental import pallas as pl
from jax.experimental.pallas import tpu as pltpu
from jax.sharding import PartitionSpec as P


BAND = 24
SUBLANES = 8
KERNEL_BYTES = 20 << 20
VMEM = pltpu.VMEM
SMEM = pltpu.SMEM


def message_order(devices):
    half = devices // 2
    across = [half ^ low for low in range(half)]
    within = list(range(1, half))
    order = across[:2]
    for pair in zip(within, across[2:]):
        order.extend(pair)
    return order + within[half - 2 :]


def filter_tile(me, tap, above, here, below, tile, tiles, rows):
    row = lax.broadcasted_iota(jnp.int32, here.shape, 0)
    column = lax.broadcasted_iota(jnp.int32, here.shape, 1)
    columns = here.shape[1]
    above = jnp.where(tile > 0, above, 0.0)
    below = jnp.where(tile < tiles - 1, below, 0.0)
    over = pltpu.roll(jnp.where(row == SUBLANES - 1, above, here), 1, 0)
    under = pltpu.roll(jnp.where(row == 0, below, here), SUBLANES - 1, 0)
    left, center, right = (
        tap[0][b] * over + tap[1][b] * here + tap[2][b] * under for b in range(3)
    )
    left = jnp.where(column == 0, 0.0, pltpu.roll(left, 1, 1))
    right = jnp.where(column == columns - 1, 0.0, pltpu.roll(right, columns - 1, 1))
    value = left + center + right
    step = rows
    while step < SUBLANES:
        swapped = jnp.where(
            (row & step) == 0,
            pltpu.roll(value, SUBLANES - step, 0),
            pltpu.roll(value, step, 0),
        )
        value = jnp.where((me * rows) & step == 0, value, swapped)
        step *= 2
    return value


def tile_rows(tile, tiles):
    spots = (jnp.maximum(tile - 1, 0), tile, jnp.minimum(tile + 1, tiles - 1))
    return [pl.ds(pl.multiple_of(spot * SUBLANES, SUBLANES), SUBLANES) for spot in spots]


def stencil_kernel(me_ref, kernel_ref, frames_ref, *refs, groups, rows, direct):
    count, height, _ = frames_ref.shape
    strips = SUBLANES // rows
    tiles = height // SUBLANES
    out_refs = refs[: len(groups) * strips]
    me = me_ref[0]
    tap = [[kernel_ref[a, b] for b in range(3)] for a in range(3)]
    if direct:
        near_ref, semaphores = refs[len(out_refs) :]
        copies = []
        for place, group in enumerate(groups):
            spans = tile_rows((me // strips) ^ group, tiles)
            for part, span in enumerate(spans):
                copies.append(
                    pltpu.make_async_copy(
                        frames_ref.at[:, span, :],
                        near_ref.at[place, part],
                        semaphores.at[place, part],
                    )
                )
        for copy in copies:
            copy.start()
        for copy in copies:
            copy.wait()
    for place, group in enumerate(groups):
        tile = (me // strips) ^ group
        spans = tile_rows(tile, tiles)
        for frame in range(count):
            if direct:
                parts = [near_ref[place, part, frame] for part in range(3)]
            else:
                parts = [frames_ref[frame, span, :] for span in spans]
            value = filter_tile(me, tap, *parts, tile, tiles, rows)
            for strip in range(strips):
                out_refs[place * strips + strip][frame * rows : (frame + 1) * rows, :] = value[
                    strip * rows : (strip + 1) * rows, :
                ]


def stencil(me, kernel, frames, groups, rows, direct):
    count, _, columns = frames.shape
    strips = SUBLANES // rows
    outs = len(groups) * strips
    size = count * rows * columns
    scratch = [
        VMEM((len(groups), 3, count, SUBLANES, columns), jnp.float32),
        pltpu.SemaphoreType.DMA((len(groups), 3)),
    ]
    return pl.pallas_call(
        functools.partial(stencil_kernel, groups=groups, rows=rows, direct=direct),
        in_specs=[
            pl.BlockSpec(memory_space=SMEM),
            pl.BlockSpec(memory_space=SMEM),
            pl.BlockSpec(memory_space=pl.ANY if direct else VMEM),
        ],
        out_specs=[pl.BlockSpec(memory_space=VMEM)] * outs,
        out_shape=[jax.ShapeDtypeStruct((count * rows, columns), jnp.float32)] * outs,
        scratch_shapes=scratch if direct else [],
        cost_estimate=pl.CostEstimate(
            flops=18 * size * outs, bytes_accessed=8 * size * outs, transcendentals=0
        ),
        compiler_params=pltpu.CompilerParams(vmem_limit_bytes=KERNEL_BYTES),
        name="stencil",
    )(me, kernel, frames)


def weights_kernel(me_ref, widths_ref, partner_ref, high_ref, low_ref, *, count, rows):
    length = widths_ref.shape[1]
    size = length * rows
    square = (length, length)
    time = lax.broadcasted_iota(jnp.int32, square, 0)
    frame = lax.rem(lax.broadcasted_iota(jnp.int32, square, 1), count)
    source = count * (me_ref[0] ^ partner_ref[...]) + frame
    spread = jnp.broadcast_to(widths_ref[...], square).T
    offset = (time - source).astype(jnp.float32)
    values = jnp.where(
        jnp.abs(offset) <= BAND, jnp.exp(-offset * offset / (2.0 * spread * spread)), 0.0
    )
    matrix = values / jnp.sum(values, axis=1, keepdims=True)
    high = matrix.astype(jnp.bfloat16)
    low = (matrix - high.astype(jnp.float32)).astype(jnp.bfloat16)

    def iota(shape, axis):
        return lax.broadcasted_iota(jnp.int32, shape, axis)

    tall, wide, full = (size, length), (length, size), (size, size)
    down = (iota(tall, 0) // rows == iota(tall, 1)).astype(jnp.bfloat16)
    along = (iota(wide, 0) == iota(wide, 1) // rows).astype(jnp.bfloat16)
    same = lax.rem(iota(full, 0), rows) == lax.rem(iota(full, 1), rows)
    dot = functools.partial(jnp.dot, preferred_element_type=jnp.float32)
    for piece, out_ref in ((high, high_ref), (low, low_ref)):
        wider = dot(down, dot(piece, along).astype(jnp.bfloat16))
        out_ref[...] = jnp.where(same, wider, 0.0).astype(jnp.bfloat16)


def spread_weights(me, widths, partners, count, rows):
    size = widths.shape[0] * rows
    columns = [partner for partner in partners for _ in range(count)]
    return pl.pallas_call(
        functools.partial(weights_kernel, count=count, rows=rows),
        in_specs=[
            pl.BlockSpec(memory_space=SMEM),
            pl.BlockSpec(memory_space=VMEM),
            pl.BlockSpec(memory_space=VMEM),
        ],
        out_specs=[pl.BlockSpec(memory_space=VMEM)] * 2,
        out_shape=[jax.ShapeDtypeStruct((size, size), jnp.bfloat16)] * 2,
        cost_estimate=pl.CostEstimate(
            flops=2 * size**3, bytes_accessed=4 * size**2, transcendentals=size
        ),
        compiler_params=pltpu.CompilerParams(vmem_limit_bytes=KERNEL_BYTES),
        name="weights",
    )(me, widths[None, :], jnp.array([columns], jnp.int32))


def product(high, low, part):
    part_high = part.astype(jnp.bfloat16)
    part_low = (part - part_high.astype(jnp.float32)).astype(jnp.bfloat16)
    dot = functools.partial(jnp.dot, preferred_element_type=jnp.float32)
    return dot(high, part_high) + dot(high, part_low) + dot(low, part_high)


def gather_kernel(high_ref, low_ref, *refs, begin, end, first, width):
    parts, out_ref = refs[:-1], refs[-1]
    if not first:
        so_far, parts = parts[0], parts[1:]
    high, low = high_ref[:, begin:end], low_ref[:, begin:end]
    for start in range(0, out_ref.shape[1], width):
        span = slice(start, start + width)
        part = jnp.concatenate([ref[:, span] for ref in parts], axis=0)
        value = product(high, low, part)
        out_ref[:, span] = value if first else so_far[:, span] + value


def last_kernel(high_ref, low_ref, *refs, begin, end, width):
    so_far, parts, out_ref = refs[0], refs[1:-1], refs[-1]
    times, rows, columns = out_ref.shape
    size = times * rows
    block = pl.ds(pl.multiple_of(pl.program_id(0) * size, size), size)
    high, low = high_ref[block, begin:end], low_ref[block, begin:end]
    for start in range(0, columns, width):
        span = slice(start, start + width)
        part = jnp.concatenate([ref[:, span] for ref in parts], axis=0)
        value = so_far[block, span] + product(high, low, part)
        out_ref[:, :, span] = value.reshape(times, rows, width)


def temporal(high, low, so_far, parts, begin, end, rows, last):
    size, columns = high.shape[0], parts[0].shape[1]
    ins = ([] if so_far is None else [so_far]) + list(parts)
    spans = dict(begin=begin, end=end, width=256)
    if last:
        shape, steps = (size // rows, rows, columns), 4
        block = (size // rows // steps, rows, columns)
        out = dict(grid=(steps,), out_specs=pl.BlockSpec(block, lambda i: (i, 0, 0)))
        body = functools.partial(last_kernel, **spans)
    else:
        shape, out = (size, columns), dict(out_specs=pl.BlockSpec(memory_space=VMEM))
        body = functools.partial(gather_kernel, first=so_far is None, **spans)
    return pl.pallas_call(
        body,
        in_specs=[pl.BlockSpec(memory_space=VMEM)] * (2 + len(ins)),
        out_shape=jax.ShapeDtypeStruct(shape, jnp.float32),
        cost_estimate=pl.CostEstimate(
            flops=6 * size * (end - begin) * columns,
            bytes_accessed=4 * size * columns * 2,
            transcendentals=0,
        ),
        compiler_params=pltpu.CompilerParams(vmem_limit_bytes=KERNEL_BYTES),
        name="temporal",
        **out,
    )(high, low, *ins)


def local(frames, widths, kernel, *, devices):
    count, height, _ = frames.shape
    rows = height // devices
    strips = SUBLANES // rows
    own = lax.axis_index("blk").astype(jnp.int32)[None]
    order = message_order(devices)
    partners = [0] + order
    every = list(dict.fromkeys(k // strips for k in order))
    messages = {}
    for stage, groups in enumerate((tuple(every[:1]), tuple(every[1:]))):
        outs = stencil(own, kernel, frames, groups, rows, stage == 0)
        for place, group in enumerate(groups):
            for strip in range(strips):
                messages[group * strips + strip] = outs[place * strips + strip]
    arrived = [messages[0]]
    for k in order:
        pairs = [(i, i ^ k) for i in range(devices)]
        arrived.append(lax.ppermute(messages[k], "blk", pairs))
    high, low = spread_weights(own, widths, partners, count, rows)
    total = None
    each = count * rows
    cuts = stage_cuts(devices)
    for begin, end in zip(cuts[:-1], cuts[1:]):
        total = temporal(
            high,
            low,
            total,
            arrived[begin:end],
            begin * each,
            end * each,
            rows,
            end == devices,
        )
    return total


def stage_cuts(devices):
    return [0, devices // 2, devices - devices // 4, devices]


def solution(mesh):
    devices = mesh.shape["blk"]
    return jax.shard_map(
        functools.partial(local, devices=devices),
        mesh=mesh,
        in_specs=(P("blk", None, None), P(), P()),
        out_specs=P(None, "blk", None),
        check_vma=False,
    )
```

```python
import functools

import jax
import jax.numpy as jnp
from jax import lax
from jax.experimental import pallas as pl
from jax.experimental.pallas import tpu as pltpu
from jax.sharding import PartitionSpec as P


BAND = 24
SUBLANES = 8
VMEM_BYTES = 67043328
KERNEL_BYTES = 20 << 20
ROOM = 256 << 10
FIRST, SECOND = 2, 2
LAST_ROWS = 64
WIDTH = 256
STEPS = 8
AHEAD = 2
VMEM = pltpu.VMEM
SMEM = pltpu.SMEM


def message_order(devices):
    half = devices // 2
    across = [half ^ low for low in range(half)]
    within = list(range(half // 2, half)) + list(range(1, half // 2))
    order = across[:AHEAD]
    for pair in zip(within, across[AHEAD:]):
        order.extend(pair)
    return order + within[half - AHEAD :]


def filter_tile(me, tap, above, here, below, tile, tiles, rows):
    row = lax.broadcasted_iota(jnp.int32, here.shape, 0)
    column = lax.broadcasted_iota(jnp.int32, here.shape, 1)
    columns = here.shape[1]
    above = jnp.where(tile > 0, above, 0.0)
    below = jnp.where(tile < tiles - 1, below, 0.0)
    over = pltpu.roll(jnp.where(row == SUBLANES - 1, above, here), 1, 0)
    under = pltpu.roll(jnp.where(row == 0, below, here), SUBLANES - 1, 0)
    left, center, right = (
        tap[0][b] * over + tap[1][b] * here + tap[2][b] * under for b in range(3)
    )
    left = jnp.where(column == 0, 0.0, pltpu.roll(left, 1, 1))
    right = jnp.where(column == columns - 1, 0.0, pltpu.roll(right, columns - 1, 1))
    value = left + center + right
    step = rows
    while step < SUBLANES:
        swapped = jnp.where(
            (row & step) == 0,
            pltpu.roll(value, SUBLANES - step, 0),
            pltpu.roll(value, step, 0),
        )
        value = jnp.where((me * rows) & step == 0, value, swapped)
        step *= 2
    return value


def tile_rows(tile, tiles):
    spots = (jnp.maximum(tile - 1, 0), tile, jnp.minimum(tile + 1, tiles - 1))
    return [pl.ds(pl.multiple_of(spot * SUBLANES, SUBLANES), SUBLANES) for spot in spots]


def stencil_kernel(kernel_ref, frames_ref, *refs, groups, rows, direct):
    count, height, _ = frames_ref.shape
    strips = SUBLANES // rows
    tiles = height // SUBLANES
    outs = len(groups) * strips
    out_refs, (tap_ref, tap_sem), scratch = refs[:outs], refs[outs : outs + 2], refs[outs + 2 :]
    me = lax.axis_index("blk")
    copies = [pltpu.make_async_copy(kernel_ref, tap_ref, tap_sem)]
    if direct:
        near_ref, near_sem = scratch
        for place, group in enumerate(groups):
            spans = tile_rows((me // strips) ^ group, tiles)
            for part, span in enumerate(spans):
                copies.append(
                    pltpu.make_async_copy(
                        frames_ref.at[:, span, :],
                        near_ref.at[place, part],
                        near_sem.at[place, part],
                    )
                )
    for copy in copies:
        copy.start()
    for copy in copies:
        copy.wait()
    tap = [[tap_ref[a, b] for b in range(3)] for a in range(3)]
    for place, group in enumerate(groups):
        tile = (me // strips) ^ group
        spans = tile_rows(tile, tiles)
        for frame in range(count):
            if direct:
                parts = [near_ref[place, part, frame] for part in range(3)]
            else:
                parts = [frames_ref[frame, span, :] for span in spans]
            value = filter_tile(me, tap, *parts, tile, tiles, rows)
            for strip in range(strips):
                out_refs[place * strips + strip][frame * rows : (frame + 1) * rows, :] = value[
                    strip * rows : (strip + 1) * rows, :
                ]


def stencil(kernel, frames, groups, rows, direct):
    count, _, columns = frames.shape
    strips = SUBLANES // rows
    outs = len(groups) * strips
    size = count * rows * columns
    scratch = [SMEM(kernel.shape, jnp.float32), pltpu.SemaphoreType.DMA]
    if direct:
        scratch += [
            VMEM((len(groups), 3, count, SUBLANES, columns), jnp.float32),
            pltpu.SemaphoreType.DMA((len(groups), 3)),
        ]
    return pl.pallas_call(
        functools.partial(stencil_kernel, groups=groups, rows=rows, direct=direct),
        in_specs=[
            pl.BlockSpec(memory_space=pltpu.HBM),
            pl.BlockSpec(memory_space=pltpu.HBM if direct else VMEM),
        ],
        out_specs=[pl.BlockSpec(memory_space=VMEM)] * outs,
        out_shape=[jax.ShapeDtypeStruct((count * rows, columns), jnp.float32)] * outs,
        scratch_shapes=scratch,
        cost_estimate=pl.CostEstimate(
            flops=18 * size * outs, bytes_accessed=8 * size * outs, transcendentals=0
        ),
        compiler_params=pltpu.CompilerParams(
            vmem_limit_bytes=VMEM_BYTES - 4 * size * outs - ROOM if direct else KERNEL_BYTES
        ),
        name="stencil",
    )(kernel, frames)


def weights_kernel(
    widths_ref, partner_ref, high_ref, low_ref, last_ref, *, count, rows
):
    length = widths_ref.shape[1]
    size = length * rows
    tail = last_ref.shape[1] // 3
    square = (length, length)

    def iota(shape, axis):
        return lax.broadcasted_iota(jnp.int32, shape, axis)

    frame = lax.rem(iota(square, 1), count)
    source = count * (lax.axis_index("blk") ^ partner_ref[...]) + frame
    spread = jnp.broadcast_to(widths_ref[...], square).T
    offset = (iota(square, 0) - source).astype(jnp.float32)
    values = jnp.where(
        jnp.abs(offset) <= BAND, jnp.exp(-offset * offset / (2.0 * spread * spread)), 0.0
    )
    matrix = values / jnp.sum(values, axis=1, keepdims=True)
    high = matrix.astype(jnp.bfloat16)
    low = (matrix - high.astype(jnp.float32)).astype(jnp.bfloat16)

    tall, wide, full = (size, length), (length, size), (size, size)
    down = (iota(tall, 0) // rows == iota(tall, 1)).astype(jnp.bfloat16)
    along = (iota(wide, 0) == iota(wide, 1) // rows).astype(jnp.bfloat16)
    same = lax.rem(iota(full, 0), rows) == lax.rem(iota(full, 1), rows)
    dot = functools.partial(jnp.dot, preferred_element_type=jnp.float32)
    for piece, out_ref in ((high, high_ref), (low, low_ref)):
        wider = dot(down, dot(piece, along).astype(jnp.bfloat16))
        out_ref[...] = jnp.where(same, wider, 0.0).astype(jnp.bfloat16)

    wide, full = (length, 3 * tail), (size, 3 * tail)
    column = size - tail + lax.rem(iota(wide, 1), tail)
    along = iota(wide, 0) == column // rows
    is_high = iota(wide, 1) < 2 * tail
    picked = dot(high, (along & is_high).astype(jnp.bfloat16)) + dot(
        low, (along & ~is_high).astype(jnp.bfloat16)
    )
    same = lax.rem(iota(full, 0), rows) == lax.rem(iota(full, 1), rows)
    wider = dot(down, picked.astype(jnp.bfloat16))
    last_ref[...] = jnp.where(same, wider, 0.0).astype(jnp.bfloat16)


def spread_weights(widths, partners, count, rows):
    size = widths.shape[0] * rows
    columns = [partner for partner in partners for _ in range(count)]
    shapes = [(size, size), (size, size), (size, 3 * LAST_ROWS)]
    return pl.pallas_call(
        functools.partial(weights_kernel, count=count, rows=rows),
        in_specs=[pl.BlockSpec(memory_space=VMEM)] * 2,
        out_specs=[pl.BlockSpec(memory_space=VMEM)] * 3,
        out_shape=[jax.ShapeDtypeStruct(shape, jnp.bfloat16) for shape in shapes],
        cost_estimate=pl.CostEstimate(
            flops=2 * size**3, bytes_accessed=4 * size**2, transcendentals=size
        ),
        compiler_params=pltpu.CompilerParams(vmem_limit_bytes=KERNEL_BYTES),
        name="weights",
    )(widths[None, :], jnp.array([columns], jnp.int32))


def split(part):
    high = part.astype(jnp.bfloat16)
    return high, (part - high.astype(jnp.float32)).astype(jnp.bfloat16)


def gather_kernel(high_ref, low_ref, *refs, begin, end, first):
    parts, out_ref = refs[:-1], refs[-1]
    if not first:
        so_far, parts = parts[0], parts[1:]
    dot = functools.partial(jnp.dot, preferred_element_type=jnp.float32)
    high, low = high_ref[:, begin:end], low_ref[:, begin:end]
    for start in range(0, out_ref.shape[1], WIDTH):
        span = slice(start, start + WIDTH)
        part_high, part_low = split(jnp.concatenate([ref[:, span] for ref in parts], axis=0))
        value = dot(high, part_high) + dot(high, part_low) + dot(low, part_high)
        out_ref[:, span] = value if first else so_far[:, span] + value


def gather(high, low, so_far, parts, begin, end):
    size, columns = high.shape[0], parts[0].shape[1]
    ins = ([] if so_far is None else [so_far]) + list(parts)
    return pl.pallas_call(
        functools.partial(gather_kernel, begin=begin, end=end, first=so_far is None),
        in_specs=[pl.BlockSpec(memory_space=VMEM)] * (2 + len(ins)),
        out_specs=pl.BlockSpec(memory_space=VMEM),
        out_shape=jax.ShapeDtypeStruct((size, columns), jnp.float32),
        cost_estimate=pl.CostEstimate(
            flops=6 * size * (end - begin) * columns,
            bytes_accessed=8 * size * columns,
            transcendentals=0,
        ),
        compiler_params=pltpu.CompilerParams(vmem_limit_bytes=KERNEL_BYTES),
        name="temporal",
    )(high, low, *ins)


def finish_kernel(weights_ref, so_far, *refs, steps):
    parts, (out_ref, done_ref, semaphores) = refs[:-3], refs[-3:]
    times, rows, columns = out_ref.shape
    step = times // steps
    part_high, part_low = split(jnp.concatenate([ref[...] for ref in parts], axis=0))
    part = jnp.concatenate([part_high, part_low, part_high], axis=0)
    copies = []
    for at in range(steps):
        span = slice(at * step * rows, (at + 1) * step * rows)
        value = jnp.dot(weights_ref[span, :], part, preferred_element_type=jnp.float32)
        done_ref[at] = (so_far[span, :] + value).reshape(step, rows, columns)
        copies.append(
            pltpu.make_async_copy(
                done_ref.at[at], out_ref.at[at * step : (at + 1) * step], semaphores.at[at]
            )
        )
        copies[-1].start()
    for copy in copies:
        copy.wait()


def finish(weights, so_far, parts, rows):
    size, columns = so_far.shape
    shape = (size // rows, rows, columns)
    return pl.pallas_call(
        functools.partial(finish_kernel, steps=STEPS),
        in_specs=[pl.BlockSpec(memory_space=VMEM)] * (2 + len(parts)),
        out_specs=pl.BlockSpec(memory_space=pltpu.HBM),
        out_shape=jax.ShapeDtypeStruct(shape, jnp.float32),
        scratch_shapes=[
            VMEM((STEPS, shape[0] // STEPS, rows, columns), jnp.float32),
            pltpu.SemaphoreType.DMA((STEPS,)),
        ],
        cost_estimate=pl.CostEstimate(
            flops=2 * size * weights.shape[1] * columns,
            bytes_accessed=8 * size * columns,
            transcendentals=0,
        ),
        compiler_params=pltpu.CompilerParams(vmem_limit_bytes=KERNEL_BYTES),
        name="finish",
    )(weights, so_far, *parts)


def local(frames, widths, kernel, *, devices):
    count, height, _ = frames.shape
    rows = height // devices
    strips = SUBLANES // rows
    order = message_order(devices)
    partners = [0] + order
    every = list(dict.fromkeys(k // strips for k in order))
    messages = {}
    ends = stencil_ends(len(every))
    for stage, (begin, end) in enumerate(zip((0,) + ends[:-1], ends)):
        groups = tuple(every[begin:end])
        outs = stencil(kernel, frames, groups, rows, stage == 0)
        for place, group in enumerate(groups):
            for strip in range(strips):
                messages[group * strips + strip] = outs[place * strips + strip]
    arrived = [messages[0]]
    for k in order:
        pairs = [(i, i ^ k) for i in range(devices)]
        arrived.append(lax.ppermute(messages[k], "blk", pairs))
    high, low, last = spread_weights(widths, partners, count, rows)
    total = None
    each = count * rows
    cuts = temporal_cuts(devices, each)
    for begin, end in zip(cuts[:-1], cuts[1:]):
        part = arrived[begin:end]
        total = gather(high, low, total, part, begin * each, end * each)
    return finish(last, total, arrived[cuts[-1] :], rows)


def stencil_ends(groups):
    return (FIRST, FIRST + SECOND, groups)


def temporal_cuts(devices, each):
    return [0, devices // 2, devices - LAST_ROWS // each]


def solution(mesh):
    devices = mesh.shape["blk"]
    return jax.shard_map(
        functools.partial(local, devices=devices),
        mesh=mesh,
        in_specs=(P("blk", None, None), P(), P()),
        out_specs=P(None, "blk", None),
        check_vma=False,
    )
```

```python
import functools

import jax
import jax.numpy as jnp
from jax import lax
from jax.experimental import pallas as pl
from jax.experimental.pallas import tpu as pltpu
from jax.sharding import PartitionSpec as P


BAND = 24
SUBLANES = 8
VMEM = pltpu.VMEM
SMEM = pltpu.SMEM
KERNEL_BYTES = 20 << 20
WIDTH = 256
STAGES = (1,)
AHEAD = 4


def message_order(devices):
    half = devices // 2
    across = [half ^ low for low in range(half)]
    within = list(range(half // 2, half)) + list(range(1, half // 2))
    order, rest = across[:AHEAD], across[AHEAD:]
    done = 0
    for at, k in enumerate(rest):
        upto = -(-(at + 1) * len(within) // len(rest))
        order += within[done:upto] + [k]
        done = upto
    return order


def filter_tile(me, tap, above, here, below, tile, tiles, rows):
    row = lax.broadcasted_iota(jnp.int32, here.shape, 0)
    column = lax.broadcasted_iota(jnp.int32, here.shape, 1)
    columns = here.shape[1]
    above = jnp.where(tile > 0, above, 0.0)
    below = jnp.where(tile < tiles - 1, below, 0.0)
    over = pltpu.roll(jnp.where(row == SUBLANES - 1, above, here), 1, 0)
    under = pltpu.roll(jnp.where(row == 0, below, here), SUBLANES - 1, 0)
    left, center, right = (
        tap[0][b] * over + tap[1][b] * here + tap[2][b] * under for b in range(3)
    )
    left = jnp.where(column == 0, 0.0, pltpu.roll(left, 1, 1))
    right = jnp.where(column == columns - 1, 0.0, pltpu.roll(right, columns - 1, 1))
    value = left + center + right
    step = rows
    while step < SUBLANES:
        swapped = jnp.where(
            (row & step) == 0,
            pltpu.roll(value, SUBLANES - step, 0),
            pltpu.roll(value, step, 0),
        )
        value = jnp.where((me * rows) & step == 0, value, swapped)
        step *= 2
    return value


def tile_rows(tile, tiles):
    spots = (jnp.maximum(tile - 1, 0), tile, jnp.minimum(tile + 1, tiles - 1))
    return [pl.ds(pl.multiple_of(spot * SUBLANES, SUBLANES), SUBLANES) for spot in spots]


def stencil_kernel(kernel_ref, frames_ref, *refs, groups, rows, direct):
    count, height, _ = frames_ref.shape
    strips = SUBLANES // rows
    tiles = height // SUBLANES
    me = lax.axis_index("blk")
    chosen = [(me // strips) ^ group for group in groups]
    spans = [tile_rows(tile, tiles) for tile in chosen]
    tap_ref, tap_sem, *near = refs[len(groups) * strips :]
    tap_copy = pltpu.make_async_copy(kernel_ref, tap_ref, tap_sem)
    tap_copy.start()
    copies = []
    if direct:
        near_ref, near_sem = near
        for place, parts in enumerate(spans):
            for part, span in enumerate(parts):
                copies.append(
                    pltpu.make_async_copy(
                        frames_ref.at[:, span, :],
                        near_ref.at[place, part],
                        near_sem.at[place, part],
                    )
                )
                copies[-1].start()
    tap_copy.wait()
    tap = [[tap_ref[a, b] for b in range(3)] for a in range(3)]
    for place, tile in enumerate(chosen):
        for copy in copies[3 * place : 3 * place + 3]:
            copy.wait()
        for frame in range(count):
            if direct:
                parts = [near_ref[place, part, frame] for part in range(3)]
            else:
                parts = [frames_ref[frame, span, :] for span in spans[place]]
            value = filter_tile(me, tap, *parts, tile, tiles, rows)
            for strip in range(strips):
                refs[place * strips + strip][frame * rows : (frame + 1) * rows, :] = value[
                    strip * rows : (strip + 1) * rows, :
                ]


def far(array):
    return pltpu.with_memory_space_constraint(array, pltpu.HBM)


def stencil(kernel, frames, groups, rows, direct):
    count, _, columns = frames.shape
    outs = len(groups) * (SUBLANES // rows)
    total = 4 * outs * count * rows * columns
    scratch = [SMEM(kernel.shape, jnp.float32), pltpu.SemaphoreType.DMA]
    if direct:
        near = (len(groups), 3, count, SUBLANES, columns)
        scratch += [VMEM(near, jnp.float32), pltpu.SemaphoreType.DMA(near[:2])]
    return pl.pallas_call(
        functools.partial(stencil_kernel, groups=groups, rows=rows, direct=direct),
        in_specs=[
            pl.BlockSpec(memory_space=pltpu.HBM),
            pl.BlockSpec(memory_space=pltpu.HBM if direct else VMEM),
        ],
        out_specs=[pl.BlockSpec(memory_space=VMEM)] * outs,
        out_shape=[jax.ShapeDtypeStruct((count * rows, columns), jnp.float32)] * outs,
        scratch_shapes=scratch,
        cost_estimate=pl.CostEstimate(
            flops=5 * total, bytes_accessed=2 * total, transcendentals=0
        ),
        compiler_params=pltpu.CompilerParams(vmem_limit_bytes=KERNEL_BYTES),
        name="stencil",
    )(far(kernel), far(frames) if direct else frames)


def weights_kernel(
    widths_ref, partner_ref, high_ref, low_ref, last_ref, *, count, rows
):
    length = widths_ref.shape[1]
    size = length * rows
    tail = last_ref.shape[1] // 3
    square = (length, length)

    def iota(shape, axis):
        return lax.broadcasted_iota(jnp.int32, shape, axis)

    frame = lax.rem(iota(square, 1), count)
    source = count * (lax.axis_index("blk") ^ partner_ref[...]) + frame
    spread = jnp.broadcast_to(widths_ref[...], square).T
    offset = (iota(square, 0) - source).astype(jnp.float32)
    values = jnp.where(
        jnp.abs(offset) <= BAND, jnp.exp(-offset * offset / (2.0 * spread * spread)), 0.0
    )
    matrix = values / jnp.sum(values, axis=1, keepdims=True)
    high = matrix.astype(jnp.bfloat16)
    low = (matrix - high.astype(jnp.float32)).astype(jnp.bfloat16)

    tall, wide, full = (size, length), (length, size), (size, size)
    down = (iota(tall, 0) // rows == iota(tall, 1)).astype(jnp.bfloat16)
    along = (iota(wide, 0) == iota(wide, 1) // rows).astype(jnp.bfloat16)
    same = lax.rem(iota(full, 0), rows) == lax.rem(iota(full, 1), rows)
    dot = functools.partial(jnp.dot, preferred_element_type=jnp.float32)
    for piece, out_ref in ((high, high_ref), (low, low_ref)):
        wider = dot(down, dot(piece, along).astype(jnp.bfloat16))
        out_ref[...] = jnp.where(same, wider, 0.0).astype(jnp.bfloat16)

    wide, full = (length, 3 * tail), (size, 3 * tail)
    column = size - tail + lax.rem(iota(wide, 1), tail)
    along = iota(wide, 0) == column // rows
    is_high = iota(wide, 1) < 2 * tail
    picked = dot(high, (along & is_high).astype(jnp.bfloat16)) + dot(
        low, (along & ~is_high).astype(jnp.bfloat16)
    )
    same = lax.rem(iota(full, 0), rows) == lax.rem(iota(full, 1), rows)
    wider = dot(down, picked.astype(jnp.bfloat16))
    last_ref[...] = jnp.where(same, wider, 0.0).astype(jnp.bfloat16)


def spread_weights(widths, partners, count, rows, tail):
    size = widths.shape[0] * rows
    columns = [partner for partner in partners for _ in range(count)]
    shapes = [(size, size), (size, size), (size, 3 * tail)]
    return pl.pallas_call(
        functools.partial(weights_kernel, count=count, rows=rows),
        in_specs=[pl.BlockSpec(memory_space=VMEM)] * 2,
        out_specs=[pl.BlockSpec(memory_space=VMEM)] * 3,
        out_shape=[jax.ShapeDtypeStruct(shape, jnp.bfloat16) for shape in shapes],
        cost_estimate=pl.CostEstimate(
            flops=2 * size**3, bytes_accessed=4 * size**2, transcendentals=size
        ),
        compiler_params=pltpu.CompilerParams(vmem_limit_bytes=KERNEL_BYTES),
        name="weights",
    )(widths[None, :], jnp.array([columns], jnp.int32))


def split(part):
    high = part.astype(jnp.bfloat16)
    return high, (part - high.astype(jnp.float32)).astype(jnp.bfloat16)


def stacked(refs, span):
    return split(jnp.concatenate([ref[:, span] for ref in refs], axis=0))


def spans_of(columns):
    return [slice(start, start + WIDTH) for start in range(0, columns, WIDTH)]


def gather_kernel(high_ref, low_ref, *refs, begin, end):
    parts, total_ref = refs[:-1], refs[-1]
    dot = functools.partial(jnp.dot, preferred_element_type=jnp.float32)
    high, low = high_ref[:, begin:end], low_ref[:, begin:end]
    for span in spans_of(total_ref.shape[1]):
        part_high, part_low = stacked(parts, span)
        total_ref[:, span] = dot(high, part_high) + dot(high, part_low) + dot(low, part_high)


def write_kernel(high_ref, low_ref, so_far_ref, *refs, begin, end):
    parts, (total_ref, out_ref, done_ref, semaphores) = refs[:-4], refs[-4:]
    dot = functools.partial(jnp.dot, preferred_element_type=jnp.float32)
    high, low = high_ref[:, begin:end], low_ref[:, begin:end]
    copies = []
    for at, span in enumerate(spans_of(total_ref.shape[1])):
        part_high, part_low = stacked(parts, span)
        value = dot(high, part_high) + dot(high, part_low) + dot(low, part_high)
        value += so_far_ref[:, span]
        total_ref[:, span] = value
        done_ref[:, :, span] = value.reshape(*done_ref.shape[:2], WIDTH)
        copies.append(
            pltpu.make_async_copy(
                done_ref.at[:, :, span], out_ref.at[:, :, span], semaphores.at[at]
            )
        )
        copies[-1].start()
    for copy in copies:
        copy.wait()


def gather(high, low, so_far, parts, begin, end, rows):
    size, columns = high.shape[0], parts[0].shape[1]
    spec = pl.BlockSpec(memory_space=VMEM)
    total = jax.ShapeDtypeStruct((size, columns), jnp.float32)
    strip = (size // rows, rows, columns)
    first = so_far is None
    if first:
        ins, outs = [high, low] + parts, dict(out_specs=spec, out_shape=total)
    else:
        ins = [high, low, so_far] + parts
        outs = dict(
            out_specs=[spec, pl.BlockSpec(memory_space=pltpu.HBM)],
            out_shape=[total, jax.ShapeDtypeStruct(strip, jnp.float32)],
            scratch_shapes=[
                VMEM(strip, jnp.float32),
                pltpu.SemaphoreType.DMA((columns // WIDTH,)),
            ],
        )
    return pl.pallas_call(
        functools.partial(gather_kernel if first else write_kernel, begin=begin, end=end),
        in_specs=[spec] * len(ins),
        cost_estimate=pl.CostEstimate(
            flops=6 * size * (end - begin) * columns,
            bytes_accessed=8 * size * columns,
            transcendentals=0,
        ),
        compiler_params=pltpu.CompilerParams(vmem_limit_bytes=KERNEL_BYTES),
        name="temporal",
        **outs,
    )(*ins)


def reach(sources):
    exact = sources % SUBLANES == 0 and BAND % SUBLANES == 0
    reached = sources + 2 * BAND + (0 if exact else SUBLANES)
    return -(-reached // SUBLANES) * SUBLANES


def finish_kernel(weights_ref, so_far_ref, _, *refs, group, sources):
    parts, (out_ref, done_ref, semaphores) = refs[:-3], refs[-3:]
    times, rows, columns = out_ref.shape
    window = done_ref.shape[0]
    strips = SUBLANES // rows
    first = ((lax.axis_index("blk") // strips) ^ group) * sources
    start = jnp.maximum(first - BAND, 0) // SUBLANES * SUBLANES
    start = jnp.minimum(start, times - window)
    block = pl.ds(pl.multiple_of(start * rows, SUBLANES * rows), window * rows)
    weights = weights_ref[block, :]
    copies = []
    for at, span in enumerate(spans_of(columns)):
        high, low = stacked(parts, span)
        part = jnp.concatenate([high, low, high], axis=0)
        value = so_far_ref[block, span] + jnp.dot(
            weights, part, preferred_element_type=jnp.float32
        )
        done_ref[:, :, span] = value.reshape(window, rows, WIDTH)
        copies.append(
            pltpu.make_async_copy(
                done_ref.at[:, :, span],
                out_ref.at[pl.ds(start, window), :, span],
                semaphores.at[at],
            )
        )
        copies[-1].start()
    for copy in copies:
        copy.wait()


def finish(weights, so_far, out, parts, group, sources):
    times, rows, columns = out.shape
    window = min(times, reach(sources))
    spec = pl.BlockSpec(memory_space=VMEM)
    far = pl.BlockSpec(memory_space=pltpu.HBM)
    return pl.pallas_call(
        functools.partial(finish_kernel, group=group, sources=sources),
        in_specs=[spec, spec, far] + [spec] * len(parts),
        out_specs=far,
        out_shape=jax.ShapeDtypeStruct(out.shape, jnp.float32),
        input_output_aliases={2: 0},
        scratch_shapes=[
            VMEM((window, rows, columns), jnp.float32),
            pltpu.SemaphoreType.DMA((columns // WIDTH,)),
        ],
        cost_estimate=pl.CostEstimate(
            flops=2 * window * rows * weights.shape[1] * columns,
            bytes_accessed=8 * window * rows * columns,
            transcendentals=0,
        ),
        compiler_params=pltpu.CompilerParams(vmem_limit_bytes=KERNEL_BYTES),
        name="finish",
    )(weights, so_far, out, *parts)


def local(frames, widths, kernel, *, devices):
    count, height, _ = frames.shape
    rows = height // devices
    strips = SUBLANES // rows
    each = count * rows
    order = message_order(devices)

    tiles = list(dict.fromkeys(k // strips for k in order))
    made = {}
    for stage, (begin, end) in enumerate(zip((0,) + STAGES, STAGES + (len(tiles),))):
        groups = tiles[begin:end]
        outs = stencil(kernel, frames, groups, rows, stage == 0)
        made.update(zip((group * strips + at for group in groups for at in range(strips)), outs))

    arrived = {0: made[0]}
    for k in order:
        arrived[k] = lax.ppermute(made[k], "blk", [(i, i ^ k) for i in range(devices)])

    group = (devices - 1) // strips
    end = [group * strips + at for at in range(strips)]
    partners = [k for k in [0] + order if k not in end] + end
    middle, tail = devices // 2, devices - strips
    high, low, final = spread_weights(widths, partners, count, rows, strips * each)
    part = [arrived[k] for k in partners]
    total = gather(high, low, None, part[:middle], 0, middle * each, rows)
    total, out = gather(high, low, total, part[middle:tail], middle * each, tail * each, rows)
    return finish(final, total, out, part[tail:], group, strips * count)


def solution(mesh):
    devices = mesh.shape["blk"]
    return jax.shard_map(
        functools.partial(local, devices=devices),
        mesh=mesh,
        in_specs=(P("blk", None, None), P(), P()),
        out_specs=P(None, "blk", None),
        check_vma=False,
    )
```

```python
import functools
import math

import jax
import jax.numpy as jnp
from jax import lax
from jax.experimental import pallas as pl
from jax.experimental.pallas import tpu as pltpu
from jax.sharding import PartitionSpec as P


BAND = 24
SUBLANES = 8
VMEM = pltpu.VMEM
SMEM = pltpu.SMEM
KERNEL_BYTES = 20 << 20
WIDTH = 256
STAGES = (1,)
LATER = 1.15
AHEAD = 4


def gray_order(count, strips):
    tiles = [tile ^ (tile >> 1) for tile in range(count // strips)]
    return [tile * strips + strip for tile in tiles for strip in range(strips)]


def message_order(devices, strips):
    half = devices // 2
    lows = gray_order(half, strips)
    across = [half ^ low for low in lows]
    within = [low for low in lows if low >= half // 2] + [k for k in lows if 0 < k < half // 2]
    order, rest = across[:AHEAD], across[AHEAD:]
    done = 0
    for at, k in enumerate(rest):
        upto = math.ceil(len(within) * ((at + 1) / len(rest)) ** LATER)
        order += within[done:upto] + [k]
        done = upto
    return order


def filter_tile(me, tap, above, here, below, tile, tiles, rows):
    row = lax.broadcasted_iota(jnp.int32, here.shape, 0)
    column = lax.broadcasted_iota(jnp.int32, here.shape, 1)
    columns = here.shape[1]
    above = jnp.where(tile > 0, above, 0.0)
    below = jnp.where(tile < tiles - 1, below, 0.0)
    over = pltpu.roll(jnp.where(row == SUBLANES - 1, above, here), 1, 0)
    under = pltpu.roll(jnp.where(row == 0, below, here), SUBLANES - 1, 0)
    left, center, right = (
        tap[0][b] * over + tap[1][b] * here + tap[2][b] * under for b in range(3)
    )
    left = jnp.where(column == 0, 0.0, pltpu.roll(left, 1, 1))
    right = jnp.where(column == columns - 1, 0.0, pltpu.roll(right, columns - 1, 1))
    value = left + center + right
    step = rows
    while step < SUBLANES:
        swapped = jnp.where(
            (row & step) == 0,
            pltpu.roll(value, SUBLANES - step, 0),
            pltpu.roll(value, step, 0),
        )
        value = jnp.where((me * rows) & step == 0, value, swapped)
        step *= 2
    return value


def tile_rows(tile, tiles):
    spots = (jnp.maximum(tile - 1, 0), tile, jnp.minimum(tile + 1, tiles - 1))
    return [pl.ds(pl.multiple_of(spot * SUBLANES, SUBLANES), SUBLANES) for spot in spots]


def stencil_kernel(kernel_ref, frames_ref, *refs, groups, rows, direct):
    count, height, _ = frames_ref.shape
    strips = SUBLANES // rows
    tiles = height // SUBLANES
    me = lax.axis_index("blk")
    chosen = [(me // strips) ^ group for group in groups]
    spans = [tile_rows(tile, tiles) for tile in chosen]
    tap_ref, tap_sem, *near = refs[len(groups) * strips :]
    tap_copy = pltpu.make_async_copy(kernel_ref, tap_ref, tap_sem)
    tap_copy.start()
    copies = []
    if direct:
        near_ref, near_sem = near
        for place, parts in enumerate(spans):
            for part, span in enumerate(parts):
                copies.append(
                    pltpu.make_async_copy(
                        frames_ref.at[:, span, :],
                        near_ref.at[place, part],
                        near_sem.at[place, part],
                    )
                )
                copies[-1].start()
    tap_copy.wait()
    tap = [[tap_ref[a, b] for b in range(3)] for a in range(3)]
    for place, tile in enumerate(chosen):
        for copy in copies[3 * place : 3 * place + 3]:
            copy.wait()
        for frame in range(count):
            if direct:
                parts = [near_ref[place, part, frame] for part in range(3)]
            else:
                parts = [frames_ref[frame, span, :] for span in spans[place]]
            value = filter_tile(me, tap, *parts, tile, tiles, rows)
            for strip in range(strips):
                refs[place * strips + strip][frame * rows : (frame + 1) * rows, :] = value[
                    strip * rows : (strip + 1) * rows, :
                ]


def far(array):
    return pltpu.with_memory_space_constraint(array, pltpu.HBM)


def stencil(kernel, frames, groups, rows, direct):
    count, _, columns = frames.shape
    outs = len(groups) * (SUBLANES // rows)
    total = 4 * outs * count * rows * columns
    scratch = [SMEM(kernel.shape, jnp.float32), pltpu.SemaphoreType.DMA]
    if direct:
        near = (len(groups), 3, count, SUBLANES, columns)
        scratch += [VMEM(near, jnp.float32), pltpu.SemaphoreType.DMA(near[:2])]
    return pl.pallas_call(
        functools.partial(stencil_kernel, groups=groups, rows=rows, direct=direct),
        in_specs=[
            pl.BlockSpec(memory_space=pltpu.HBM),
            pl.BlockSpec(memory_space=pltpu.HBM if direct else VMEM),
        ],
        out_specs=[pl.BlockSpec(memory_space=VMEM)] * outs,
        out_shape=[jax.ShapeDtypeStruct((count * rows, columns), jnp.float32)] * outs,
        scratch_shapes=scratch,
        cost_estimate=pl.CostEstimate(
            flops=5 * total, bytes_accessed=2 * total, transcendentals=0
        ),
        compiler_params=pltpu.CompilerParams(vmem_limit_bytes=KERNEL_BYTES),
        name="stencil",
    )(far(kernel), far(frames) if direct else frames)


def weights_kernel(
    widths_ref, partner_ref, high_ref, low_ref, last_ref, *, count, rows
):
    length = widths_ref.shape[1]
    size = length * rows
    tail = last_ref.shape[1] // 3
    square = (length, length)

    def iota(shape, axis):
        return lax.broadcasted_iota(jnp.int32, shape, axis)

    frame = lax.rem(iota(square, 1), count)
    source = count * (lax.axis_index("blk") ^ partner_ref[...]) + frame
    spread = jnp.broadcast_to(widths_ref[...], square).T
    offset = (iota(square, 0) - source).astype(jnp.float32)
    values = jnp.where(
        jnp.abs(offset) <= BAND, jnp.exp(-offset * offset / (2.0 * spread * spread)), 0.0
    )
    matrix = values / jnp.sum(values, axis=1, keepdims=True)
    high = matrix.astype(jnp.bfloat16)
    low = (matrix - high.astype(jnp.float32)).astype(jnp.bfloat16)

    tall, wide, full = (size, length), (length, size), (size, size)
    down = (iota(tall, 0) // rows == iota(tall, 1)).astype(jnp.bfloat16)
    along = (iota(wide, 0) == iota(wide, 1) // rows).astype(jnp.bfloat16)
    same = lax.rem(iota(full, 0), rows) == lax.rem(iota(full, 1), rows)
    dot = functools.partial(jnp.dot, preferred_element_type=jnp.float32)
    for piece, out_ref in ((high, high_ref), (low, low_ref)):
        wider = dot(down, dot(piece, along).astype(jnp.bfloat16))
        out_ref[...] = jnp.where(same, wider, 0.0).astype(jnp.bfloat16)

    wide, full = (length, 3 * tail), (size, 3 * tail)
    column = size - tail + lax.rem(iota(wide, 1), tail)
    along = iota(wide, 0) == column // rows
    is_high = iota(wide, 1) < 2 * tail
    picked = dot(high, (along & is_high).astype(jnp.bfloat16)) + dot(
        low, (along & ~is_high).astype(jnp.bfloat16)
    )
    same = lax.rem(iota(full, 0), rows) == lax.rem(iota(full, 1), rows)
    wider = dot(down, picked.astype(jnp.bfloat16))
    last_ref[...] = jnp.where(same, wider, 0.0).astype(jnp.bfloat16)


def spread_weights(widths, partners, count, rows, tail):
    size = widths.shape[0] * rows
    columns = [partner for partner in partners for _ in range(count)]
    shapes = [(size, size), (size, size), (size, 3 * tail)]
    return pl.pallas_call(
        functools.partial(weights_kernel, count=count, rows=rows),
        in_specs=[pl.BlockSpec(memory_space=VMEM)] * 2,
        out_specs=[pl.BlockSpec(memory_space=VMEM)] * 3,
        out_shape=[jax.ShapeDtypeStruct(shape, jnp.bfloat16) for shape in shapes],
        cost_estimate=pl.CostEstimate(
            flops=2 * size**3, bytes_accessed=4 * size**2, transcendentals=size
        ),
        compiler_params=pltpu.CompilerParams(vmem_limit_bytes=KERNEL_BYTES),
        name="weights",
    )(widths[None, :], jnp.array([columns], jnp.int32))


def split(part):
    high = part.astype(jnp.bfloat16)
    return high, (part - high.astype(jnp.float32)).astype(jnp.bfloat16)


def stacked(refs, span):
    return split(jnp.concatenate([ref[:, span] for ref in refs], axis=0))


def spans_of(columns):
    return [slice(start, start + WIDTH) for start in range(0, columns, WIDTH)]


def gather_kernel(high_ref, low_ref, *refs, begin, end):
    parts, total_ref = refs[:-1], refs[-1]
    dot = functools.partial(jnp.dot, preferred_element_type=jnp.float32)
    high, low = high_ref[:, begin:end], low_ref[:, begin:end]
    for span in spans_of(total_ref.shape[1]):
        part_high, part_low = stacked(parts, span)
        total_ref[:, span] = dot(high, part_high) + dot(high, part_low) + dot(low, part_high)


def write_kernel(high_ref, low_ref, so_far_ref, *refs, begin, end):
    parts, (total_ref, out_ref, done_ref, semaphores) = refs[:-4], refs[-4:]
    dot = functools.partial(jnp.dot, preferred_element_type=jnp.float32)
    high, low = high_ref[:, begin:end], low_ref[:, begin:end]
    copies = []
    for at, span in enumerate(spans_of(total_ref.shape[1])):
        part_high, part_low = stacked(parts, span)
        value = dot(high, part_high) + dot(high, part_low) + dot(low, part_high)
        value += so_far_ref[:, span]
        total_ref[:, span] = value
        done_ref[:, :, span] = value.reshape(*done_ref.shape[:2], WIDTH)
        copies.append(
            pltpu.make_async_copy(
                done_ref.at[:, :, span], out_ref.at[:, :, span], semaphores.at[at]
            )
        )
        copies[-1].start()
    for copy in copies:
        copy.wait()


def gather(high, low, so_far, parts, begin, end, rows):
    size, columns = high.shape[0], parts[0].shape[1]
    spec = pl.BlockSpec(memory_space=VMEM)
    total = jax.ShapeDtypeStruct((size, columns), jnp.float32)
    strip = (size // rows, rows, columns)
    first = so_far is None
    if first:
        ins, outs = [high, low] + parts, dict(out_specs=spec, out_shape=total)
    else:
        ins = [high, low, so_far] + parts
        outs = dict(
            out_specs=[spec, pl.BlockSpec(memory_space=pltpu.HBM)],
            out_shape=[total, jax.ShapeDtypeStruct(strip, jnp.float32)],
            scratch_shapes=[
                VMEM(strip, jnp.float32),
                pltpu.SemaphoreType.DMA((columns // WIDTH,)),
            ],
        )
    return pl.pallas_call(
        functools.partial(gather_kernel if first else write_kernel, begin=begin, end=end),
        in_specs=[spec] * len(ins),
        cost_estimate=pl.CostEstimate(
            flops=6 * size * (end - begin) * columns,
            bytes_accessed=8 * size * columns,
            transcendentals=0,
        ),
        compiler_params=pltpu.CompilerParams(vmem_limit_bytes=KERNEL_BYTES),
        name="temporal",
        **outs,
    )(*ins)


def reach(sources):
    exact = sources % SUBLANES == 0 and BAND % SUBLANES == 0
    reached = sources + 2 * BAND + (0 if exact else SUBLANES)
    return -(-reached // SUBLANES) * SUBLANES


def finish_kernel(weights_ref, so_far_ref, _, *refs, group, sources):
    parts, (out_ref, done_ref, semaphores) = refs[:-3], refs[-3:]
    times, rows, columns = out_ref.shape
    window = done_ref.shape[0]
    strips = SUBLANES // rows
    first = ((lax.axis_index("blk") // strips) ^ group) * sources
    start = jnp.maximum(first - BAND, 0) // SUBLANES * SUBLANES
    start = jnp.minimum(start, times - window)
    block = pl.ds(pl.multiple_of(start * rows, SUBLANES * rows), window * rows)
    weights = weights_ref[block, :]
    copies = []
    for at, span in enumerate(spans_of(columns)):
        high, low = stacked(parts, span)
        part = jnp.concatenate([high, low, high], axis=0)
        value = so_far_ref[block, span] + jnp.dot(
            weights, part, preferred_element_type=jnp.float32
        )
        done_ref[:, :, span] = value.reshape(window, rows, WIDTH)
        copies.append(
            pltpu.make_async_copy(
                done_ref.at[:, :, span],
                out_ref.at[pl.ds(start, window), :, span],
                semaphores.at[at],
            )
        )
        copies[-1].start()
    for copy in copies:
        copy.wait()


def finish(weights, so_far, out, parts, group, sources):
    times, rows, columns = out.shape
    window = min(times, reach(sources))
    spec = pl.BlockSpec(memory_space=VMEM)
    far = pl.BlockSpec(memory_space=pltpu.HBM)
    return pl.pallas_call(
        functools.partial(finish_kernel, group=group, sources=sources),
        in_specs=[spec, spec, far] + [spec] * len(parts),
        out_specs=far,
        out_shape=jax.ShapeDtypeStruct(out.shape, jnp.float32),
        input_output_aliases={2: 0},
        scratch_shapes=[
            VMEM((window, rows, columns), jnp.float32),
            pltpu.SemaphoreType.DMA((columns // WIDTH,)),
        ],
        cost_estimate=pl.CostEstimate(
            flops=2 * window * rows * weights.shape[1] * columns,
            bytes_accessed=8 * window * rows * columns,
            transcendentals=0,
        ),
        compiler_params=pltpu.CompilerParams(vmem_limit_bytes=KERNEL_BYTES),
        name="finish",
    )(weights, so_far, out, *parts)


def local(frames, widths, kernel, *, devices):
    count, height, _ = frames.shape
    rows = height // devices
    strips = SUBLANES // rows
    each = count * rows
    order = message_order(devices, strips)

    tiles = list(dict.fromkeys(k // strips for k in order))
    made = {}
    for stage, (begin, end) in enumerate(zip((0,) + STAGES, STAGES + (len(tiles),))):
        groups = tiles[begin:end]
        outs = stencil(kernel, frames, groups, rows, stage == 0)
        made.update(zip((group * strips + at for group in groups for at in range(strips)), outs))

    arrived = {0: made[0]}
    for k in order:
        arrived[k] = lax.ppermute(made[k], "blk", [(i, i ^ k) for i in range(devices)])

    group = order[-1] // strips
    end = [group * strips + at for at in range(strips)]
    partners = [k for k in [0] + order if k not in end] + end
    middle, tail = devices // 2, devices - strips
    high, low, final = spread_weights(widths, partners, count, rows, strips * each)
    part = [arrived[k] for k in partners]
    total = gather(high, low, None, part[:middle], 0, middle * each, rows)
    total, out = gather(high, low, total, part[middle:tail], middle * each, tail * each, rows)
    return finish(final, total, out, part[tail:], group, strips * count)


def solution(mesh):
    devices = mesh.shape["blk"]
    return jax.shard_map(
        functools.partial(local, devices=devices),
        mesh=mesh,
        in_specs=(P("blk", None, None), P(), P()),
        out_specs=P(None, "blk", None),
        check_vma=False,
    )
```

```python
import functools
import math

import jax
import jax.numpy as jnp
from jax import lax
from jax.experimental import pallas as pl
from jax.experimental.pallas import tpu as pltpu
from jax.sharding import PartitionSpec as P


BAND = 24
SUBLANES = 8
VMEM = pltpu.VMEM
SMEM = pltpu.SMEM
KERNEL_BYTES = 20 << 20
WIDTH = 256
STAGES = (1,)
LATER = 1.25
AHEAD = 4


def gray_order(count, strips):
    tiles = [tile ^ (tile >> 1) for tile in range(count // strips)]
    return [tile * strips + strip for tile in tiles for strip in range(strips)]


def message_order(devices, strips):
    half = devices // 2
    lows = gray_order(half, strips)
    across = [half ^ low for low in lows]
    within = [low for low in lows if low >= half // 2] + [k for k in lows if 0 < k < half // 2]
    order, rest = across[:AHEAD], across[AHEAD:]
    done = 0
    for at, k in enumerate(rest):
        upto = math.ceil(len(within) * ((at + 1) / len(rest)) ** LATER)
        order += within[done:upto] + [k]
        done = upto
    return order


def filter_tile(me, tap, above, here, below, tile, tiles, rows):
    row = lax.broadcasted_iota(jnp.int32, here.shape, 0)
    column = lax.broadcasted_iota(jnp.int32, here.shape, 1)
    columns = here.shape[1]
    above = jnp.where(tile > 0, above, 0.0)
    below = jnp.where(tile < tiles - 1, below, 0.0)
    over = pltpu.roll(jnp.where(row == SUBLANES - 1, above, here), 1, 0)
    under = pltpu.roll(jnp.where(row == 0, below, here), SUBLANES - 1, 0)
    left, center, right = (
        tap[0][b] * over + tap[1][b] * here + tap[2][b] * under for b in range(3)
    )
    left = jnp.where(column == 0, 0.0, pltpu.roll(left, 1, 1))
    right = jnp.where(column == columns - 1, 0.0, pltpu.roll(right, columns - 1, 1))
    value = left + center + right
    step = rows
    while step < SUBLANES:
        swapped = jnp.where(
            (row & step) == 0,
            pltpu.roll(value, SUBLANES - step, 0),
            pltpu.roll(value, step, 0),
        )
        value = jnp.where((me * rows) & step == 0, value, swapped)
        step *= 2
    return value


def tile_rows(tile, tiles, base=0):
    spots = (jnp.maximum(tile - 1, 0), tile, jnp.minimum(tile + 1, tiles - 1))
    return [
        pl.ds(pl.multiple_of((spot - base) * SUBLANES, SUBLANES), SUBLANES) for spot in spots
    ]


def stencil_kernel(kernel_ref, frames_ref, *refs, groups, rows, direct):
    count, height, _ = frames_ref.shape
    strips = SUBLANES // rows
    tiles = height // SUBLANES
    me = lax.axis_index("blk")
    chosen = [(me // strips) ^ group for group in groups]
    spans = [tile_rows(tile, tiles) for tile in chosen]
    tap_ref, tap_sem, *near = refs[len(groups) * strips :]
    tap_copy = pltpu.make_async_copy(kernel_ref, tap_ref, tap_sem)
    tap_copy.start()
    copies = []
    if direct:
        near_ref, near_sem = near
        base = [jnp.clip(tile - 1, 0, tiles - 3) for tile in chosen]
        for place, first in enumerate(base):
            span = pl.ds(pl.multiple_of(first * SUBLANES, SUBLANES), 3 * SUBLANES)
            copies.append(
                pltpu.make_async_copy(
                    frames_ref.at[:, span, :], near_ref.at[place], near_sem.at[place]
                )
            )
            copies[-1].start()
    tap_copy.wait()
    tap = [[tap_ref[a, b] for b in range(3)] for a in range(3)]
    for place, tile in enumerate(chosen):
        for copy in copies[place : place + 1]:
            copy.wait()
        for frame in range(count):
            if direct:
                at = tile_rows(tile, tiles, base[place])
                parts = [near_ref[place, frame, span, :] for span in at]
            else:
                parts = [frames_ref[frame, span, :] for span in spans[place]]
            value = filter_tile(me, tap, *parts, tile, tiles, rows)
            for strip in range(strips):
                refs[place * strips + strip][frame * rows : (frame + 1) * rows, :] = value[
                    strip * rows : (strip + 1) * rows, :
                ]


def far(array):
    return pltpu.with_memory_space_constraint(array, pltpu.HBM)


def stencil(kernel, frames, groups, rows, direct):
    count, _, columns = frames.shape
    outs = len(groups) * (SUBLANES // rows)
    total = 4 * outs * count * rows * columns
    scratch = [SMEM(kernel.shape, jnp.float32), pltpu.SemaphoreType.DMA]
    if direct:
        near = (len(groups), count, 3 * SUBLANES, columns)
        scratch += [VMEM(near, jnp.float32), pltpu.SemaphoreType.DMA(near[:1])]
    return pl.pallas_call(
        functools.partial(stencil_kernel, groups=groups, rows=rows, direct=direct),
        in_specs=[
            pl.BlockSpec(memory_space=pltpu.HBM),
            pl.BlockSpec(memory_space=pltpu.HBM if direct else VMEM),
        ],
        out_specs=[pl.BlockSpec(memory_space=VMEM)] * outs,
        out_shape=[jax.ShapeDtypeStruct((count * rows, columns), jnp.float32)] * outs,
        scratch_shapes=scratch,
        cost_estimate=pl.CostEstimate(
            flops=5 * total, bytes_accessed=2 * total, transcendentals=0
        ),
        compiler_params=pltpu.CompilerParams(vmem_limit_bytes=KERNEL_BYTES),
        name="stencil",
    )(far(kernel), far(frames) if direct else frames)


def weights_kernel(
    widths_ref, partner_ref, high_ref, low_ref, last_ref, *, count, rows
):
    length = widths_ref.shape[1]
    size = length * rows
    tail = last_ref.shape[1] // 3
    square = (length, length)

    def iota(shape, axis):
        return lax.broadcasted_iota(jnp.int32, shape, axis)

    frame = lax.rem(iota(square, 1), count)
    source = count * (lax.axis_index("blk") ^ partner_ref[...]) + frame
    spread = jnp.broadcast_to(widths_ref[...], square).T
    offset = (iota(square, 0) - source).astype(jnp.float32)
    values = jnp.where(
        jnp.abs(offset) <= BAND, jnp.exp(-offset * offset / (2.0 * spread * spread)), 0.0
    )
    matrix = values / jnp.sum(values, axis=1, keepdims=True)
    high = matrix.astype(jnp.bfloat16)
    low = (matrix - high.astype(jnp.float32)).astype(jnp.bfloat16)

    tall, wide, full = (size, length), (length, size), (size, size)
    down = (iota(tall, 0) // rows == iota(tall, 1)).astype(jnp.bfloat16)
    along = (iota(wide, 0) == iota(wide, 1) // rows).astype(jnp.bfloat16)
    same = lax.rem(iota(full, 0), rows) == lax.rem(iota(full, 1), rows)
    dot = functools.partial(jnp.dot, preferred_element_type=jnp.float32)
    for piece, out_ref in ((high, high_ref), (low, low_ref)):
        wider = dot(down, dot(piece, along).astype(jnp.bfloat16))
        out_ref[...] = jnp.where(same, wider, 0.0).astype(jnp.bfloat16)

    wide, full = (length, 3 * tail), (size, 3 * tail)
    column = size - tail + lax.rem(iota(wide, 1), tail)
    along = iota(wide, 0) == column // rows
    is_high = iota(wide, 1) < 2 * tail
    picked = dot(high, (along & is_high).astype(jnp.bfloat16)) + dot(
        low, (along & ~is_high).astype(jnp.bfloat16)
    )
    same = lax.rem(iota(full, 0), rows) == lax.rem(iota(full, 1), rows)
    wider = dot(down, picked.astype(jnp.bfloat16))
    last_ref[...] = jnp.where(same, wider, 0.0).astype(jnp.bfloat16)


def spread_weights(widths, partners, count, rows, tail):
    size = widths.shape[0] * rows
    columns = [partner for partner in partners for _ in range(count)]
    shapes = [(size, size), (size, size), (size, 3 * tail)]
    return pl.pallas_call(
        functools.partial(weights_kernel, count=count, rows=rows),
        in_specs=[pl.BlockSpec(memory_space=VMEM)] * 2,
        out_specs=[pl.BlockSpec(memory_space=VMEM)] * 3,
        out_shape=[jax.ShapeDtypeStruct(shape, jnp.bfloat16) for shape in shapes],
        cost_estimate=pl.CostEstimate(
            flops=2 * size**3, bytes_accessed=4 * size**2, transcendentals=size
        ),
        compiler_params=pltpu.CompilerParams(vmem_limit_bytes=KERNEL_BYTES),
        name="weights",
    )(widths[None, :], jnp.array([columns], jnp.int32))


def split(part):
    high = part.astype(jnp.bfloat16)
    return high, (part - high.astype(jnp.float32)).astype(jnp.bfloat16)


def stacked(refs, span):
    return split(jnp.concatenate([ref[:, span] for ref in refs], axis=0))


def spans_of(columns):
    return [slice(start, start + WIDTH) for start in range(0, columns, WIDTH)]


def gather_kernel(high_ref, low_ref, *refs, begin, end):
    parts, total_ref = refs[:-1], refs[-1]
    dot = functools.partial(jnp.dot, preferred_element_type=jnp.float32)
    high, low = high_ref[:, begin:end], low_ref[:, begin:end]
    for span in spans_of(total_ref.shape[1]):
        part_high, part_low = stacked(parts, span)
        total_ref[:, span] = dot(high, part_high) + dot(high, part_low) + dot(low, part_high)


def write_kernel(high_ref, low_ref, so_far_ref, *refs, begin, end):
    parts, (total_ref, out_ref, done_ref, semaphores) = refs[:-4], refs[-4:]
    dot = functools.partial(jnp.dot, preferred_element_type=jnp.float32)
    high, low = high_ref[:, begin:end], low_ref[:, begin:end]
    copies = []
    for at, span in enumerate(spans_of(total_ref.shape[1])):
        part_high, part_low = stacked(parts, span)
        value = dot(high, part_high) + dot(high, part_low) + dot(low, part_high)
        value += so_far_ref[:, span]
        total_ref[:, span] = value
        done_ref[:, :, span] = value.reshape(*done_ref.shape[:2], WIDTH)
        copies.append(
            pltpu.make_async_copy(
                done_ref.at[:, :, span], out_ref.at[:, :, span], semaphores.at[at]
            )
        )
        copies[-1].start()
    for copy in copies:
        copy.wait()


def gather(high, low, so_far, parts, begin, end, rows):
    size, columns = high.shape[0], parts[0].shape[1]
    spec = pl.BlockSpec(memory_space=VMEM)
    total = jax.ShapeDtypeStruct((size, columns), jnp.float32)
    strip = (size // rows, rows, columns)
    first = so_far is None
    if first:
        ins, outs = [high, low] + parts, dict(out_specs=spec, out_shape=total)
    else:
        ins = [high, low, so_far] + parts
        outs = dict(
            out_specs=[spec, pl.BlockSpec(memory_space=pltpu.HBM)],
            out_shape=[total, jax.ShapeDtypeStruct(strip, jnp.float32)],
            scratch_shapes=[
                VMEM(strip, jnp.float32),
                pltpu.SemaphoreType.DMA((columns // WIDTH,)),
            ],
        )
    return pl.pallas_call(
        functools.partial(gather_kernel if first else write_kernel, begin=begin, end=end),
        in_specs=[spec] * len(ins),
        cost_estimate=pl.CostEstimate(
            flops=6 * size * (end - begin) * columns,
            bytes_accessed=8 * size * columns,
            transcendentals=0,
        ),
        compiler_params=pltpu.CompilerParams(vmem_limit_bytes=KERNEL_BYTES),
        name="temporal",
        **outs,
    )(*ins)


def reach(sources):
    exact = sources % SUBLANES == 0 and BAND % SUBLANES == 0
    reached = sources + 2 * BAND + (0 if exact else SUBLANES)
    return -(-reached // SUBLANES) * SUBLANES


def finish_kernel(weights_ref, so_far_ref, _, *refs, group, sources):
    parts, (out_ref, done_ref, semaphores) = refs[:-3], refs[-3:]
    times, rows, columns = out_ref.shape
    window = done_ref.shape[0]
    strips = SUBLANES // rows
    first = ((lax.axis_index("blk") // strips) ^ group) * sources
    start = jnp.maximum(first - BAND, 0) // SUBLANES * SUBLANES
    start = jnp.minimum(start, times - window)
    block = pl.ds(pl.multiple_of(start * rows, SUBLANES * rows), window * rows)
    weights = weights_ref[block, :]
    copies = []
    for at, span in enumerate(spans_of(columns)):
        high, low = stacked(parts, span)
        part = jnp.concatenate([high, low, high], axis=0)
        value = so_far_ref[block, span] + jnp.dot(
            weights, part, preferred_element_type=jnp.float32
        )
        done_ref[:, :, span] = value.reshape(window, rows, WIDTH)
        copies.append(
            pltpu.make_async_copy(
                done_ref.at[:, :, span],
                out_ref.at[pl.ds(start, window), :, span],
                semaphores.at[at],
            )
        )
        copies[-1].start()
    for copy in copies:
        copy.wait()


def finish(weights, so_far, out, parts, group, sources):
    times, rows, columns = out.shape
    window = min(times, reach(sources))
    spec = pl.BlockSpec(memory_space=VMEM)
    far = pl.BlockSpec(memory_space=pltpu.HBM)
    return pl.pallas_call(
        functools.partial(finish_kernel, group=group, sources=sources),
        in_specs=[spec, spec, far] + [spec] * len(parts),
        out_specs=far,
        out_shape=jax.ShapeDtypeStruct(out.shape, jnp.float32),
        input_output_aliases={2: 0},
        scratch_shapes=[
            VMEM((window, rows, columns), jnp.float32),
            pltpu.SemaphoreType.DMA((columns // WIDTH,)),
        ],
        cost_estimate=pl.CostEstimate(
            flops=2 * window * rows * weights.shape[1] * columns,
            bytes_accessed=8 * window * rows * columns,
            transcendentals=0,
        ),
        compiler_params=pltpu.CompilerParams(vmem_limit_bytes=KERNEL_BYTES),
        name="finish",
    )(weights, so_far, out, *parts)


def local(frames, widths, kernel, *, devices):
    count, height, _ = frames.shape
    rows = height // devices
    strips = SUBLANES // rows
    each = count * rows
    order = message_order(devices, strips)

    tiles = list(dict.fromkeys(k // strips for k in order))
    made = {}
    for stage, (begin, end) in enumerate(zip((0,) + STAGES, STAGES + (len(tiles),))):
        groups = tiles[begin:end]
        outs = stencil(kernel, frames, groups, rows, stage == 0)
        made.update(zip((group * strips + at for group in groups for at in range(strips)), outs))

    arrived = {0: made[0]}
    for k in order:
        arrived[k] = lax.ppermute(made[k], "blk", [(i, i ^ k) for i in range(devices)])

    group = order[-1] // strips
    end = [group * strips + at for at in range(strips)]
    partners = [k for k in [0] + order if k not in end] + end
    middle, tail = devices // 2, devices - strips
    high, low, final = spread_weights(widths, partners, count, rows, strips * each)
    part = [arrived[k] for k in partners]
    total = gather(high, low, None, part[:middle], 0, middle * each, rows)
    total, out = gather(high, low, total, part[middle:tail], middle * each, tail * each, rows)
    return finish(final, total, out, part[tail:], group, strips * count)


def solution(mesh):
    devices = mesh.shape["blk"]
    return jax.shard_map(
        functools.partial(local, devices=devices),
        mesh=mesh,
        in_specs=(P("blk", None, None), P(), P()),
        out_specs=P(None, "blk", None),
        check_vma=False,
    )
```

```python
import functools
import math

import jax
import jax.numpy as jnp
from jax import lax
from jax.experimental import pallas as pl
from jax.experimental.pallas import tpu as pltpu
from jax.sharding import PartitionSpec as P


BAND = 24
SUBLANES = 8
VMEM = pltpu.VMEM
SMEM = pltpu.SMEM
KERNEL_BYTES = 20 << 20
FIRST_BYTES = 56000000
WIDTH = 256
STAGES = (1,)
LATER = 1.25
AHEAD = 4


def gray_order(count, strips):
    tiles = [tile ^ (tile >> 1) for tile in range(count // strips)]
    return [tile * strips + strip for tile in tiles for strip in range(strips)]


def message_order(devices, strips):
    half = devices // 2
    lows = gray_order(half, strips)
    across = [half ^ low for low in lows]
    within = [low for low in lows if low >= half // 2] + [
        k for k in lows[::-1] if 0 < k < half // 2
    ]
    order, rest = across[:AHEAD], across[AHEAD:]
    done = 0
    for at, k in enumerate(rest):
        upto = math.ceil(len(within) * ((at + 1) / len(rest)) ** LATER)
        order += within[done:upto] + [k]
        done = upto
    return order


def filter_tile(me, tap, above, here, below, tile, tiles, rows):
    row = lax.broadcasted_iota(jnp.int32, here.shape, 0)
    column = lax.broadcasted_iota(jnp.int32, here.shape, 1)
    columns = here.shape[1]
    above = jnp.where(tile > 0, above, 0.0)
    below = jnp.where(tile < tiles - 1, below, 0.0)
    over = pltpu.roll(jnp.where(row == SUBLANES - 1, above, here), 1, 0)
    under = pltpu.roll(jnp.where(row == 0, below, here), SUBLANES - 1, 0)
    left, center, right = (
        tap[0][b] * over + tap[1][b] * here + tap[2][b] * under for b in range(3)
    )
    left = jnp.where(column == 0, 0.0, pltpu.roll(left, 1, 1))
    right = jnp.where(column == columns - 1, 0.0, pltpu.roll(right, columns - 1, 1))
    value = left + center + right
    step = rows
    while step < SUBLANES:
        swapped = jnp.where(
            (row & step) == 0,
            pltpu.roll(value, SUBLANES - step, 0),
            pltpu.roll(value, step, 0),
        )
        value = jnp.where((me * rows) & step == 0, value, swapped)
        step *= 2
    return value


def tile_rows(tile, tiles, base=0):
    spots = (jnp.maximum(tile - 1, 0), tile, jnp.minimum(tile + 1, tiles - 1))
    return [
        pl.ds(pl.multiple_of((spot - base) * SUBLANES, SUBLANES), SUBLANES) for spot in spots
    ]


def stencil_kernel(kernel_ref, frames_ref, *refs, groups, rows, direct):
    count, height, _ = frames_ref.shape
    strips = SUBLANES // rows
    tiles = height // SUBLANES
    me = lax.axis_index("blk")
    chosen = [(me // strips) ^ group for group in groups]
    spans = [tile_rows(tile, tiles) for tile in chosen]
    tap_ref, tap_sem, *near = refs[len(groups) * strips :]
    tap_copy = pltpu.make_async_copy(kernel_ref, tap_ref, tap_sem)
    tap_copy.start()
    copies = []
    if direct:
        near_ref, near_sem = near
        base = [jnp.clip(tile - 1, 0, tiles - 3) for tile in chosen]
        for place, first in enumerate(base):
            span = pl.ds(pl.multiple_of(first * SUBLANES, SUBLANES), 3 * SUBLANES)
            copies.append(
                pltpu.make_async_copy(
                    frames_ref.at[:, span, :], near_ref.at[place], near_sem.at[place]
                )
            )
            copies[-1].start()
    tap_copy.wait()
    tap = [[tap_ref[a, b] for b in range(3)] for a in range(3)]
    for place, tile in enumerate(chosen):
        for copy in copies[place : place + 1]:
            copy.wait()
        for frame in range(count):
            if direct:
                at = tile_rows(tile, tiles, base[place])
                parts = [near_ref[place, frame, span, :] for span in at]
            else:
                parts = [frames_ref[frame, span, :] for span in spans[place]]
            value = filter_tile(me, tap, *parts, tile, tiles, rows)
            for strip in range(strips):
                refs[place * strips + strip][frame * rows : (frame + 1) * rows, :] = value[
                    strip * rows : (strip + 1) * rows, :
                ]


def far(array):
    return pltpu.with_memory_space_constraint(array, pltpu.HBM)


def stencil(kernel, frames, groups, rows, direct):
    count, _, columns = frames.shape
    outs = len(groups) * (SUBLANES // rows)
    total = 4 * outs * count * rows * columns
    scratch = [SMEM(kernel.shape, jnp.float32), pltpu.SemaphoreType.DMA]
    if direct:
        near = (len(groups), count, 3 * SUBLANES, columns)
        scratch += [VMEM(near, jnp.float32), pltpu.SemaphoreType.DMA(near[:1])]
    return pl.pallas_call(
        functools.partial(stencil_kernel, groups=groups, rows=rows, direct=direct),
        in_specs=[
            pl.BlockSpec(memory_space=pltpu.HBM),
            pl.BlockSpec(memory_space=pltpu.HBM if direct else VMEM),
        ],
        out_specs=[pl.BlockSpec(memory_space=VMEM)] * outs,
        out_shape=[jax.ShapeDtypeStruct((count * rows, columns), jnp.float32)] * outs,
        scratch_shapes=scratch,
        cost_estimate=pl.CostEstimate(
            flops=5 * total, bytes_accessed=2 * total, transcendentals=0
        ),
        compiler_params=pltpu.CompilerParams(vmem_limit_bytes=FIRST_BYTES - total if direct else KERNEL_BYTES),
        name="stencil",
    )(far(kernel), far(frames) if direct else frames)


def weights_kernel(
    widths_ref, partner_ref, high_ref, low_ref, last_ref, *, count, rows
):
    length = widths_ref.shape[1]
    size = length * rows
    tail = last_ref.shape[1] // 3
    square = (length, length)

    def iota(shape, axis):
        return lax.broadcasted_iota(jnp.int32, shape, axis)

    frame = lax.rem(iota(square, 1), count)
    source = count * (lax.axis_index("blk") ^ partner_ref[...]) + frame
    spread = jnp.broadcast_to(widths_ref[...], square).T
    offset = (iota(square, 0) - source).astype(jnp.float32)
    values = jnp.where(
        jnp.abs(offset) <= BAND, jnp.exp(-offset * offset / (2.0 * spread * spread)), 0.0
    )
    matrix = values / jnp.sum(values, axis=1, keepdims=True)
    high = matrix.astype(jnp.bfloat16)
    low = (matrix - high.astype(jnp.float32)).astype(jnp.bfloat16)

    tall, wide, full = (size, length), (length, size), (size, size)
    down = (iota(tall, 0) // rows == iota(tall, 1)).astype(jnp.bfloat16)
    along = (iota(wide, 0) == iota(wide, 1) // rows).astype(jnp.bfloat16)
    same = lax.rem(iota(full, 0), rows) == lax.rem(iota(full, 1), rows)
    dot = functools.partial(jnp.dot, preferred_element_type=jnp.float32)
    for piece, out_ref in ((high, high_ref), (low, low_ref)):
        wider = dot(down, dot(piece, along).astype(jnp.bfloat16))
        out_ref[...] = jnp.where(same, wider, 0.0).astype(jnp.bfloat16)

    wide, full = (length, 3 * tail), (size, 3 * tail)
    column = size - tail + lax.rem(iota(wide, 1), tail)
    along = iota(wide, 0) == column // rows
    is_high = iota(wide, 1) < 2 * tail
    picked = dot(high, (along & is_high).astype(jnp.bfloat16)) + dot(
        low, (along & ~is_high).astype(jnp.bfloat16)
    )
    same = lax.rem(iota(full, 0), rows) == lax.rem(iota(full, 1), rows)
    wider = dot(down, picked.astype(jnp.bfloat16))
    last_ref[...] = jnp.where(same, wider, 0.0).astype(jnp.bfloat16)


def spread_weights(widths, partners, count, rows, tail):
    size = widths.shape[0] * rows
    columns = [partner for partner in partners for _ in range(count)]
    shapes = [(size, size), (size, size), (size, 3 * tail)]
    return pl.pallas_call(
        functools.partial(weights_kernel, count=count, rows=rows),
        in_specs=[pl.BlockSpec(memory_space=VMEM)] * 2,
        out_specs=[pl.BlockSpec(memory_space=VMEM)] * 3,
        out_shape=[jax.ShapeDtypeStruct(shape, jnp.bfloat16) for shape in shapes],
        cost_estimate=pl.CostEstimate(
            flops=2 * size**3, bytes_accessed=4 * size**2, transcendentals=size
        ),
        compiler_params=pltpu.CompilerParams(vmem_limit_bytes=KERNEL_BYTES),
        name="weights",
    )(widths[None, :], jnp.array([columns], jnp.int32))


def split(part):
    high = part.astype(jnp.bfloat16)
    return high, (part - high.astype(jnp.float32)).astype(jnp.bfloat16)


def stacked(refs, span):
    return split(jnp.concatenate([ref[:, span] for ref in refs], axis=0))


def spans_of(columns):
    return [slice(start, start + WIDTH) for start in range(0, columns, WIDTH)]


def gather_kernel(high_ref, low_ref, *refs, begin, end):
    parts, total_ref = refs[:-1], refs[-1]
    dot = functools.partial(jnp.dot, preferred_element_type=jnp.float32)
    high, low = high_ref[:, begin:end], low_ref[:, begin:end]
    for span in spans_of(total_ref.shape[1]):
        part_high, part_low = stacked(parts, span)
        total_ref[:, span] = dot(high, part_high) + dot(high, part_low) + dot(low, part_high)


def write_kernel(high_ref, low_ref, so_far_ref, *refs, begin, end):
    parts, (total_ref, out_ref, done_ref, semaphores) = refs[:-4], refs[-4:]
    dot = functools.partial(jnp.dot, preferred_element_type=jnp.float32)
    high, low = high_ref[:, begin:end], low_ref[:, begin:end]
    copies = []
    for at, span in enumerate(spans_of(total_ref.shape[1])):
        part_high, part_low = stacked(parts, span)
        value = dot(high, part_high) + dot(high, part_low) + dot(low, part_high)
        value += so_far_ref[:, span]
        total_ref[:, span] = value
        done_ref[:, :, span] = value.reshape(*done_ref.shape[:2], WIDTH)
        copies.append(
            pltpu.make_async_copy(
                done_ref.at[:, :, span], out_ref.at[:, :, span], semaphores.at[at]
            )
        )
        copies[-1].start()
    for copy in copies:
        copy.wait()


def gather(high, low, so_far, parts, begin, end, rows):
    size, columns = high.shape[0], parts[0].shape[1]
    spec = pl.BlockSpec(memory_space=VMEM)
    total = jax.ShapeDtypeStruct((size, columns), jnp.float32)
    strip = (size // rows, rows, columns)
    first = so_far is None
    if first:
        ins, outs = [high, low] + parts, dict(out_specs=spec, out_shape=total)
    else:
        ins = [high, low, so_far] + parts
        outs = dict(
            out_specs=[spec, pl.BlockSpec(memory_space=pltpu.HBM)],
            out_shape=[total, jax.ShapeDtypeStruct(strip, jnp.float32)],
            scratch_shapes=[
                VMEM(strip, jnp.float32),
                pltpu.SemaphoreType.DMA((columns // WIDTH,)),
            ],
        )
    return pl.pallas_call(
        functools.partial(gather_kernel if first else write_kernel, begin=begin, end=end),
        in_specs=[spec] * len(ins),
        cost_estimate=pl.CostEstimate(
            flops=6 * size * (end - begin) * columns,
            bytes_accessed=8 * size * columns,
            transcendentals=0,
        ),
        compiler_params=pltpu.CompilerParams(vmem_limit_bytes=KERNEL_BYTES),
        name="temporal",
        **outs,
    )(*ins)


def reach(sources):
    exact = sources % SUBLANES == 0 and BAND % SUBLANES == 0
    reached = sources + 2 * BAND + (0 if exact else SUBLANES)
    return -(-reached // SUBLANES) * SUBLANES


def finish_kernel(weights_ref, so_far_ref, _, *refs, group, sources):
    parts, (out_ref, done_ref, semaphores) = refs[:-3], refs[-3:]
    times, rows, columns = out_ref.shape
    window = done_ref.shape[0]
    strips = SUBLANES // rows
    first = ((lax.axis_index("blk") // strips) ^ group) * sources
    start = jnp.maximum(first - BAND, 0) // SUBLANES * SUBLANES
    start = jnp.minimum(start, times - window)
    block = pl.ds(pl.multiple_of(start * rows, SUBLANES * rows), window * rows)
    weights = weights_ref[block, :]
    copies = []
    for at, span in enumerate(spans_of(columns)):
        high, low = stacked(parts, span)
        part = jnp.concatenate([high, low, high], axis=0)
        value = so_far_ref[block, span] + jnp.dot(
            weights, part, preferred_element_type=jnp.float32
        )
        done_ref[:, :, span] = value.reshape(window, rows, WIDTH)
        copies.append(
            pltpu.make_async_copy(
                done_ref.at[:, :, span],
                out_ref.at[pl.ds(start, window), :, span],
                semaphores.at[at],
            )
        )
        copies[-1].start()
    for copy in copies:
        copy.wait()


def finish(weights, so_far, out, parts, group, sources):
    times, rows, columns = out.shape
    window = min(times, reach(sources))
    spec = pl.BlockSpec(memory_space=VMEM)
    far = pl.BlockSpec(memory_space=pltpu.HBM)
    return pl.pallas_call(
        functools.partial(finish_kernel, group=group, sources=sources),
        in_specs=[spec, spec, far] + [spec] * len(parts),
        out_specs=far,
        out_shape=jax.ShapeDtypeStruct(out.shape, jnp.float32),
        input_output_aliases={2: 0},
        scratch_shapes=[
            VMEM((window, rows, columns), jnp.float32),
            pltpu.SemaphoreType.DMA((columns // WIDTH,)),
        ],
        cost_estimate=pl.CostEstimate(
            flops=2 * window * rows * weights.shape[1] * columns,
            bytes_accessed=8 * window * rows * columns,
            transcendentals=0,
        ),
        compiler_params=pltpu.CompilerParams(vmem_limit_bytes=KERNEL_BYTES),
        name="finish",
    )(weights, so_far, out, *parts)


def local(frames, widths, kernel, *, devices):
    count, height, _ = frames.shape
    rows = height // devices
    strips = SUBLANES // rows
    each = count * rows
    order = message_order(devices, strips)

    tiles = list(dict.fromkeys(k // strips for k in order))
    made = {}
    for stage, (begin, end) in enumerate(zip((0,) + STAGES, STAGES + (len(tiles),))):
        groups = tiles[begin:end]
        outs = stencil(kernel, frames, groups, rows, stage == 0)
        made.update(zip((group * strips + at for group in groups for at in range(strips)), outs))

    arrived = {0: made[0]}
    for k in order:
        arrived[k] = lax.ppermute(made[k], "blk", [(i, i ^ k) for i in range(devices)])

    group = order[-1] // strips
    end = [group * strips + at for at in range(strips)]
    partners = [k for k in [0] + order if k not in end] + end
    middle, tail = devices // 2, devices - strips
    high, low, final = spread_weights(widths, partners, count, rows, strips * each)
    part = [arrived[k] for k in partners]
    total = gather(high, low, None, part[:middle], 0, middle * each, rows)
    total, out = gather(high, low, total, part[middle:tail], middle * each, tail * each, rows)
    return finish(final, total, out, part[tail:], group, strips * count)


def solution(mesh):
    devices = mesh.shape["blk"]
    return jax.shard_map(
        functools.partial(local, devices=devices),
        mesh=mesh,
        in_specs=(P("blk", None, None), P(), P()),
        out_specs=P(None, "blk", None),
        check_vma=False,
    )
```
